32 devices in a mesh: outer: 4 (over y, x), dev: 8 (over z, core).
Axes of the slice: x: 2, y: 2, z: 4, core: 2. Of those that a mesh axis runs over, the one named last changes fastest.
Arguments:
- documents: bfloat16 [6144, 4096], P(('outer', 'dev')), may hold values from -8 to 8
- cluster_of: int32 [6144], replicated, may hold values from 0 to 31, as said below
- neighbours: int32 [32, 4], replicated, may hold values from 0 to 31, as said below
- sharpness: float32 [32], replicated, may hold values from 32 to 64
Outputs:
- density: float32 [6144], P(('outer', 'dev'))
The draws below stay inside these ranges and needn't reach their ends.
Inputs may be any that keep to these rules, and one draw needn't show every extreme that they name: `cluster_of`: rows b * 192 to (b + 1) * 192 - 1 form block b. Block b names only clusters g * 8 to (g + 1) * 8 - 1, with g = b // 8, and names no cluster more than 48 times; in each group g some cluster is named exactly 48 times by every block of that group; every cluster is named by some row. `neighbours`: row c, with c = g * 8 + h, lists in order the clusters g * 8 + ((h - 1) mod 8), g * 8 + ((h + 1) mod 8), ((g - 1) mod 4) * 8 + ((h + b) mod 8) and ((g + 1) mod 4) * 8 + ((h + d) mod 8), with b and d each in -1, 0, 1.
All inputs are finite; a program needn't handle non-finite values.
Results may differ from the reference program's by a relative error of at most 0.00047.
Values may be sent and summed in bfloat16 or wider, within the bound.
A program may use at most 128 MiB of HBM per device.

```python
import math
import jax
import jax.numpy as jnp
from jax import lax

E = 4096
NEIGHBOURS = 4
TOK_DEV = 192
CLUSTER_GROUPS = 4
CLUSTERS_IN_GROUP = 8
CLUSTERS = 32
CAP = 48
SLOTS = 384
DOCS = 6144


theme_count = 32


def cluster_draw(key):
    blocks_total = CLUSTER_GROUPS * CLUSTERS_IN_GROUP
    tickets = CLUSTERS_IN_GROUP * CAP
    base_key = jax.random.fold_in(key, 7)
    split_points = jax.random.split(base_key, 4)
    extra_reward = jax.random.randint(split_points[0], (CLUSTER_GROUPS, CLUSTERS_IN_GROUP), 0, 4096)
    weighty_blocks = jax.random.randint(split_points[1], (CLUSTER_GROUPS,), 0, CLUSTERS_IN_GROUP)
    extra_reward = jnp.where(jnp.arange(CLUSTERS_IN_GROUP, dtype=jnp.int32)[None, :] == weighty_blocks[:, None], 32768, extra_reward)
    owner_of_ticket = jnp.arange(tickets, dtype=jnp.int32) // CAP
    ticket_copy = jnp.arange(tickets, dtype=jnp.int32) % CAP
    random_perturb = jax.random.randint(split_points[2], (blocks_total, tickets), 0, 4096)
    group_of_block = jnp.arange(blocks_total, dtype=jnp.int32) // CLUSTERS_IN_GROUP
    block_owner = jnp.arange(blocks_total, dtype=jnp.int32) % CLUSTERS_IN_GROUP
    compelled_choice = (owner_of_ticket[None, :] == block_owner[:, None]) & (ticket_copy[None, :] == 0)
    density_scores = random_perturb + extra_reward[group_of_block][:, owner_of_ticket] + jnp.where(compelled_choice, 65536, 0)
    density_scores = density_scores * tickets + jnp.arange(tickets, dtype=jnp.int32)[None, :]
    ranked, chosen = lax.top_k(density_scores, TOK_DEV)
    local_labels = owner_of_ticket[chosen]
    shuffled = jax.random.permutation(split_points[3], local_labels, axis=1, independent=True)
    labels_all = shuffled + group_of_block[:, None] * CLUSTERS_IN_GROUP
    return labels_all.reshape(-1).astype(jnp.int32)


def draw_cluster_of(key, part):
    return cluster_draw(key)


def draw_documents(key, part):
    labels_all = cluster_draw(key)
    base_key = jax.random.fold_in(key, 13)
    split_points = jax.random.split(base_key, 4)
    centres = jax.random.normal(split_points[0], (CLUSTERS, E), jnp.float32)
    themes = jax.random.normal(split_points[1], (theme_count, E), jnp.float32)
    picked = jax.random.randint(split_points[2], (DOCS,), 0, theme_count)
    noise = jax.random.normal(split_points[3], (DOCS, E), jnp.float32)
    theme_weight = 0.35
    values = centres[labels_all] + theme_weight * themes[picked] + noise
    return jnp.clip(values, -8.0, 8.0).astype(jnp.bfloat16)


def draw_neighbours(key, part):
    base_key = jax.random.fold_in(key, 17)
    offsets = jax.random.randint(base_key, (CLUSTERS, 2), -1, 2).astype(jnp.int32)
    cluster_range = jnp.arange(CLUSTERS, dtype=jnp.int32)
    group_of = cluster_range // CLUSTERS_IN_GROUP
    owner_of = cluster_range % CLUSTERS_IN_GROUP
    group_moves = jnp.stack([jnp.zeros_like(group_of), jnp.zeros_like(group_of), jnp.full_like(group_of, -1), jnp.ones_like(group_of)], axis=1)
    owner_moves = jnp.stack([jnp.full_like(owner_of, -1), jnp.ones_like(owner_of), offsets[:, 0], offsets[:, 1]], axis=1)
    group_next = (group_of[:, None] + group_moves + CLUSTER_GROUPS) % CLUSTER_GROUPS
    owner_next = (owner_of[:, None] + owner_moves + CLUSTERS_IN_GROUP) % CLUSTERS_IN_GROUP
    return (group_next * CLUSTERS_IN_GROUP + owner_next).astype(jnp.int32)


def setup_inputs(seed: int = 0) -> dict:
    key_of = jax.random.split(jax.random.key(seed), 5)
    return {
        "documents": draw_documents(jax.random.fold_in(key_of[4], 71), 0),
        "cluster_of": draw_cluster_of(jax.random.fold_in(key_of[4], 71), 0),
        "neighbours": draw_neighbours(jax.random.fold_in(key_of[4], 71), 0),
        "sharpness": jnp.clip(jnp.exp(jax.random.uniform(key_of[3], (CLUSTERS,), jnp.float32, math.log(32.0), math.log(64.0))), 32.0, 64.0),
    }


def reference(documents, cluster_of, neighbours, sharpness):
    count_blocks = DOCS // TOK_DEV
    cluster_sizes = jnp.zeros((CLUSTERS,), jnp.int32).at[cluster_of].add(1)
    cluster_sums = jax.ops.segment_sum(documents.astype(jnp.float32), cluster_of, num_segments=CLUSTERS)
    cluster_means = cluster_sums / cluster_sizes.astype(jnp.float32)[:, None]
    centred = documents.astype(jnp.float32) - cluster_means[cluster_of]
    scaling = lax.rsqrt(lax.optimization_barrier(jnp.mean(centred * centred, axis=1)) + 1e-06) / math.sqrt(E)
    unit_rows = (centred * scaling[:, None]).astype(jnp.bfloat16)
    block_labels = cluster_of.reshape(count_blocks, TOK_DEV)
    ordinal = jnp.arange(TOK_DEV, dtype=jnp.int32)
    earlier = ordinal[None, :] < ordinal[:, None]
    repeats = lax.optimization_barrier(jnp.sum(((block_labels[:, :, None] == block_labels[:, None, :]) & earlier[None]).astype(jnp.int32), axis=2))
    source_slot = (jnp.arange(count_blocks, dtype=jnp.int32) % CLUSTERS_IN_GROUP)[:, None]
    slot_of = (source_slot * CAP + repeats).reshape(-1).astype(jnp.int32)
    rows_index = jnp.arange(DOCS, dtype=jnp.int32)
    slot_table = jnp.zeros((CLUSTERS, SLOTS), jnp.int32).at[cluster_of, slot_of].set(rows_index)
    filled = jnp.zeros((CLUSTERS, SLOTS), jnp.float32).at[cluster_of, slot_of].set(1.0)
    off_diagonal = 1.0 - jnp.eye(SLOTS, dtype=jnp.float32)

    def per_cluster(cluster_index):
        queries = unit_rows[slot_table[cluster_index]]
        own_gain = sharpness[cluster_index]
        own_terms = jnp.exp(own_gain * jnp.dot(queries, queries.T, preferred_element_type=jnp.float32))
        running = lax.optimization_barrier(jnp.sum(own_terms * filled[cluster_index][None, :] * off_diagonal, axis=1))
        for position in range(NEIGHBOURS):
            partner = neighbours[cluster_index, position]
            key_rows = unit_rows[slot_table[partner]]
            pair_gain = 0.5 * (own_gain + sharpness[partner])
            kernel_terms = jnp.exp(pair_gain * jnp.dot(queries, key_rows.T, preferred_element_type=jnp.float32))
            running = running + lax.optimization_barrier(jnp.sum(kernel_terms * filled[partner][None, :], axis=1))
        partner_count = cluster_sizes[cluster_index] - 1 + jnp.sum(cluster_sizes[neighbours[cluster_index]])
        return jnp.log(running / partner_count.astype(jnp.float32))
    slot_density = lax.map(per_cluster, jnp.arange(CLUSTERS, dtype=jnp.int32))
    return slot_density[cluster_of, slot_of]
```

```python
import math

import jax
import jax.numpy as jnp
from jax import lax
from jax.sharding import PartitionSpec as P


def passed_along(block, axis, distance):
    devices = range(lax.axis_size(axis))
    route = [((i - distance) % len(devices), i) for i in devices]
    return lax.ppermute(block, axis, route)


def kernel_block(queries, others, pair_gain):
    products = jnp.einsum("qe,ke->qk", queries, others, preferred_element_type=jnp.float32)
    return jnp.exp(pair_gain * products)


def shards(documents, cluster_of, neighbours, sharpness):
    groups = lax.axis_size("outer")
    owners = lax.axis_size("dev")
    tokens_here = documents.shape[0]
    feature_width = documents.shape[1]
    capacity = max(2, 2 * tokens_here // owners)
    slot_count = owners * capacity
    group_index = lax.axis_index("outer")
    owner_index = lax.axis_index("dev")
    own_cluster = group_index * owners + owner_index
    block_labels = cluster_of.reshape(groups * owners, tokens_here)
    group_of_block = jnp.arange(groups * owners, dtype=jnp.int32) // owners
    local_labels = block_labels - group_of_block[:, None] * owners
    owner_range = jnp.arange(owners, dtype=jnp.int32)
    per_block = jnp.sum(
        (local_labels[:, :, None] == owner_range).astype(jnp.int32), axis=1
    ).reshape(groups, owners, owners)
    cluster_sizes = jnp.sum(per_block, axis=1).reshape(-1)
    own_labels = lax.dynamic_index_in_dim(local_labels, own_cluster, 0, keepdims=False)
    ordinal = jnp.arange(tokens_here, dtype=jnp.int32)
    earlier = ordinal[None, :] < ordinal[:, None]
    repeats = jnp.sum(
        ((own_labels[:, None] == own_labels[None, :]) & earlier).astype(jnp.int32), axis=1
    )
    target = own_labels * capacity + repeats
    placing = (jnp.arange(slot_count, dtype=jnp.int32)[:, None] == target[None, :]).astype(
        jnp.bfloat16
    )
    outgoing = jnp.dot(placing, documents, preferred_element_type=jnp.float32).astype(jnp.bfloat16)
    arrived = lax.all_to_all(
        outgoing.reshape(owners, capacity, feature_width),
        "dev",
        split_axis=0,
        concat_axis=0,
        tiled=True,
    ).reshape(slot_count, feature_width)

    def slot_mask(group_at, owner_at):
        senders = per_block[group_at, :, owner_at]
        return (
            (jnp.arange(capacity, dtype=jnp.int32)[None, :] < senders[:, None])
            .astype(jnp.float32)
            .reshape(-1)
        )

    present = slot_mask(group_index, owner_index)
    centre = jnp.dot(
        present.astype(jnp.bfloat16)[None, :], arrived, preferred_element_type=jnp.float32
    )[0]
    centre = centre / cluster_sizes[own_cluster].astype(jnp.float32)
    centred = arrived.astype(jnp.float32) - centre[None, :]
    scaling = lax.rsqrt(jnp.mean(centred * centred, axis=1) + 1e-06) / math.sqrt(feature_width)
    unit_rows = (centred * (scaling * present)[:, None]).astype(jnp.bfloat16)
    own_gain = sharpness[own_cluster]
    listed = neighbours[own_cluster]
    off_diagonal = 1.0 - jnp.eye(slot_count, dtype=jnp.float32)
    running = jnp.sum(
        kernel_block(unit_rows, unit_rows, own_gain) * (present[None, :] * off_diagonal), axis=1
    )
    beside = [passed_along(unit_rows, "dev", offset) for offset in (1, -1)]
    vertical = []
    for direction, position in ((1, 2), (-1, 3)):
        receiver_group = (group_index + direction) % groups
        wanted = neighbours[receiver_group * owners + owner_index, position]
        delta = (wanted % owners - owner_index + owners) % owners
        picked_rows = jnp.where(
            delta == 1, beside[1], jnp.where(delta == owners - 1, beside[0], unit_rows)
        )
        vertical.append(passed_along(picked_rows, "outer", direction))
    key_sets = [beside[0], beside[1], vertical[0], vertical[1]]
    for position in range(4):
        partner = listed[position]
        partner_group_at = partner // owners
        partner_owner_at = partner % owners
        partner_partner = partner_group_at * owners + partner_owner_at
        pair_gain = 0.5 * (own_gain + sharpness[partner_partner])
        partner = partner_partner
        kernel_terms = kernel_block(unit_rows, key_sets[position], pair_gain)
        key_mask = slot_mask(partner_group_at, partner_owner_at)
        running = running + jnp.sum(kernel_terms * key_mask[None, :], axis=1)
    partner_count = cluster_sizes[own_cluster] - 1 + jnp.sum(cluster_sizes[listed])
    slot_density = jnp.log(running / partner_count.astype(jnp.float32))
    answered = lax.all_to_all(
        slot_density.reshape(owners, capacity), "dev", split_axis=0, concat_axis=0, tiled=True
    ).reshape(-1)
    return answered[target]


def lookup(table, index):
    hit = index[:, None] == jnp.arange(table.shape[0], dtype=jnp.int32)[None, :]
    return jnp.sum(jnp.where(hit, table[None, :], jnp.zeros((), table.dtype)), axis=1)


def gathered(documents, cluster_of, neighbours, sharpness):
    groups = lax.axis_size("outer")
    owners = lax.axis_size("dev")
    tokens_here, feature_width = documents.shape
    group_index = lax.axis_index("outer")
    owner_index = lax.axis_index("dev")
    clusters = groups * owners
    group_rows = owners * tokens_here
    cluster_range = jnp.arange(clusters, dtype=jnp.int32)
    sizes = jnp.sum((cluster_of[:, None] == cluster_range[None, :]).astype(jnp.int32), axis=0)

    def labels_at(group_at):
        start = (group_at * owners + owner_index) * tokens_here
        return lax.dynamic_slice_in_dim(cluster_of, start, tokens_here)

    previous = (group_index + groups - 1) % groups
    following = (group_index + 1) % groups
    own = labels_at(group_index)
    local = own - group_index * owners
    local_range = jnp.arange(owners, dtype=jnp.int32)
    member = (local_range[:, None] == local[None, :]).astype(jnp.bfloat16)
    sums = lax.psum(jnp.dot(member, documents, preferred_element_type=jnp.float32), "dev")
    own_sizes = lax.dynamic_slice_in_dim(sizes, group_index * owners, owners)
    means = sums / own_sizes.astype(jnp.float32)[:, None]
    centre = jnp.dot(
        member.astype(jnp.float32).T,
        means,
        precision=lax.Precision.HIGHEST,
        preferred_element_type=jnp.float32,
    )
    centred = documents.astype(jnp.float32) - centre
    scaling = lax.rsqrt(jnp.mean(centred * centred, axis=1) + 1e-06) / math.sqrt(feature_width)
    unit_rows = (centred * scaling[:, None]).astype(jnp.bfloat16)
    from_previous = passed_along(unit_rows, "outer", 1)
    from_following = passed_along(unit_rows, "outer", -1)
    keys = lax.all_gather(unit_rows, "dev", axis=0, tiled=True)
    key_labels = lax.dynamic_slice_in_dim(cluster_of, group_index * group_rows, group_rows)
    key_gain = lookup(sharpness, key_labels)

    def partial(queries, labels, positions, own_too):
        products = jnp.einsum("qe,ke->qk", queries, keys, preferred_element_type=jnp.float32)
        gain = 0.5 * (lookup(sharpness, labels)[:, None] + key_gain[None, :])
        wanted = jnp.zeros(products.shape, jnp.bool_)
        for position in positions:
            listed = lookup(neighbours[:, position], labels)
            wanted = wanted | (listed[:, None] == key_labels[None, :])
        if own_too:
            at = owner_index * tokens_here + jnp.arange(tokens_here, dtype=jnp.int32)
            other = at[:, None] != jnp.arange(group_rows, dtype=jnp.int32)[None, :]
            wanted = wanted | ((labels[:, None] == key_labels[None, :]) & other)
        return jnp.sum(jnp.where(wanted, jnp.exp(gain * products), 0.0), axis=1)

    back_previous = partial(from_previous, labels_at(previous), (3,), False)
    back_following = partial(from_following, labels_at(following), (2,), False)
    running = partial(unit_rows, own, (0, 1), True)
    running = running + passed_along(back_previous, "outer", -1)
    running = running + passed_along(back_following, "outer", 1)
    counts = sizes - 1
    for position in range(neighbours.shape[1]):
        counts = counts + lookup(sizes, neighbours[:, position])
    return jnp.log(running / lookup(counts, own).astype(jnp.float32))


def solution(mesh):
    small = mesh.shape["dev"] <= 8
    in_specs = (P(("outer", "dev"), None), P(), P(), P())
    out_specs = P(("outer", "dev"))
    body = gathered if small else shards
    return jax.shard_map(body, mesh=mesh, in_specs=in_specs, out_specs=out_specs, check_vma=False)
```

```python
import functools
import math

import jax
import jax.numpy as jnp
from jax import lax
from jax.experimental import pallas as pl
from jax.experimental.pallas import tpu as pltpu
from jax.sharding import PartitionSpec as P


def passed_along(block, axis, distance):
    devices = range(lax.axis_size(axis))
    route = [((i - distance) % len(devices), i) for i in devices]
    return lax.ppermute(block, axis, route)


def kernel_block(queries, others, pair_gain):
    products = jnp.einsum("qe,ke->qk", queries, others, preferred_element_type=jnp.float32)
    return jnp.exp(pair_gain * products)


def shards(documents, cluster_of, neighbours, sharpness):
    groups = lax.axis_size("outer")
    owners = lax.axis_size("dev")
    tokens_here = documents.shape[0]
    feature_width = documents.shape[1]
    capacity = max(2, 2 * tokens_here // owners)
    slot_count = owners * capacity
    group_index = lax.axis_index("outer")
    owner_index = lax.axis_index("dev")
    own_cluster = group_index * owners + owner_index
    block_labels = cluster_of.reshape(groups * owners, tokens_here)
    group_of_block = jnp.arange(groups * owners, dtype=jnp.int32) // owners
    local_labels = block_labels - group_of_block[:, None] * owners
    owner_range = jnp.arange(owners, dtype=jnp.int32)
    per_block = jnp.sum(
        (local_labels[:, :, None] == owner_range).astype(jnp.int32), axis=1
    ).reshape(groups, owners, owners)
    cluster_sizes = jnp.sum(per_block, axis=1).reshape(-1)
    own_labels = lax.dynamic_index_in_dim(local_labels, own_cluster, 0, keepdims=False)
    ordinal = jnp.arange(tokens_here, dtype=jnp.int32)
    earlier = ordinal[None, :] < ordinal[:, None]
    repeats = jnp.sum(
        ((own_labels[:, None] == own_labels[None, :]) & earlier).astype(jnp.int32), axis=1
    )
    target = own_labels * capacity + repeats
    placing = (jnp.arange(slot_count, dtype=jnp.int32)[:, None] == target[None, :]).astype(
        jnp.bfloat16
    )
    outgoing = jnp.dot(placing, documents, preferred_element_type=jnp.float32).astype(jnp.bfloat16)
    arrived = lax.all_to_all(
        outgoing.reshape(owners, capacity, feature_width),
        "dev",
        split_axis=0,
        concat_axis=0,
        tiled=True,
    ).reshape(slot_count, feature_width)

    def slot_mask(group_at, owner_at):
        senders = per_block[group_at, :, owner_at]
        return (
            (jnp.arange(capacity, dtype=jnp.int32)[None, :] < senders[:, None])
            .astype(jnp.float32)
            .reshape(-1)
        )

    present = slot_mask(group_index, owner_index)
    centre = jnp.dot(
        present.astype(jnp.bfloat16)[None, :], arrived, preferred_element_type=jnp.float32
    )[0]
    centre = centre / cluster_sizes[own_cluster].astype(jnp.float32)
    centred = arrived.astype(jnp.float32) - centre[None, :]
    scaling = lax.rsqrt(jnp.mean(centred * centred, axis=1) + 1e-06) / math.sqrt(feature_width)
    unit_rows = (centred * (scaling * present)[:, None]).astype(jnp.bfloat16)
    own_gain = sharpness[own_cluster]
    listed = neighbours[own_cluster]
    off_diagonal = 1.0 - jnp.eye(slot_count, dtype=jnp.float32)
    running = jnp.sum(
        kernel_block(unit_rows, unit_rows, own_gain) * (present[None, :] * off_diagonal), axis=1
    )
    beside = [passed_along(unit_rows, "dev", offset) for offset in (1, -1)]
    vertical = []
    for direction, position in ((1, 2), (-1, 3)):
        receiver_group = (group_index + direction) % groups
        wanted = neighbours[receiver_group * owners + owner_index, position]
        delta = (wanted % owners - owner_index + owners) % owners
        picked_rows = jnp.where(
            delta == 1, beside[1], jnp.where(delta == owners - 1, beside[0], unit_rows)
        )
        vertical.append(passed_along(picked_rows, "outer", direction))
    key_sets = [beside[0], beside[1], vertical[0], vertical[1]]
    for position in range(4):
        partner = listed[position]
        partner_group_at = partner // owners
        partner_owner_at = partner % owners
        partner_partner = partner_group_at * owners + partner_owner_at
        pair_gain = 0.5 * (own_gain + sharpness[partner_partner])
        partner = partner_partner
        kernel_terms = kernel_block(unit_rows, key_sets[position], pair_gain)
        key_mask = slot_mask(partner_group_at, partner_owner_at)
        running = running + jnp.sum(kernel_terms * key_mask[None, :], axis=1)
    partner_count = cluster_sizes[own_cluster] - 1 + jnp.sum(cluster_sizes[listed])
    slot_density = jnp.log(running / partner_count.astype(jnp.float32))
    answered = lax.all_to_all(
        slot_density.reshape(owners, capacity), "dev", split_axis=0, concat_axis=0, tiled=True
    ).reshape(-1)
    return answered[target]


MESH = pl.DeviceIdType.MESH


def meet(peers, expected):
    barrier = pltpu.get_barrier_semaphore()
    for present, peer in peers:
        if present is None:
            pl.semaphore_signal(barrier, inc=1, device_id=peer, device_id_type=MESH)
        else:

            @pl.when(present)
            def _(peer=peer):
                pl.semaphore_signal(barrier, inc=1, device_id=peer, device_id_type=MESH)

    pl.semaphore_wait(barrier, expected)


def sum_kernel(owners, part_ref, out_ref, landed, reduced, gathered_sums, sems):
    me = lax.axis_index("dev")
    width = part_ref.shape[1] // owners

    def span(at):
        return pl.ds(pl.multiple_of(at * width, 128), width)

    others = [lax.rem(me + step, owners) for step in range(1, owners)]
    meet([(None, {"dev": peer}) for peer in others], owners - 1)

    def scatter(step):
        return pltpu.make_async_remote_copy(
            src_ref=part_ref.at[:, span(others[step])],
            dst_ref=landed.at[step],
            send_sem=sems.at[0, step],
            recv_sem=sems.at[1, step],
            device_id={"dev": others[step]},
            device_id_type=MESH,
        )

    def spread(step):
        return pltpu.make_async_remote_copy(
            src_ref=reduced,
            dst_ref=gathered_sums.at[step],
            send_sem=sems.at[2, step],
            recv_sem=sems.at[3, step],
            device_id={"dev": others[step]},
            device_id_type=MESH,
        )

    for step in range(owners - 1):
        scatter(step).start()
    total = part_ref[:, span(me)]
    for step in range(owners - 1):
        scatter(step).wait_recv()
        total = total + landed[step]
    reduced[...] = total
    for step in range(owners - 1):
        spread(step).start()
    out_ref[:, span(me)] = total
    for step in range(owners - 1):
        spread(step).wait_recv()
        sender = lax.rem(me + owners - 1 - step, owners)
        out_ref[:, span(sender)] = gathered_sums[step]
    for step in range(owners - 1):
        scatter(step).wait_send()
        spread(step).wait_send()


def summed(part):
    owners = lax.axis_size("dev")
    rows, width = part.shape
    block = (owners - 1, rows, width // owners)
    return pl.pallas_call(
        functools.partial(sum_kernel, owners),
        out_shape=jax.ShapeDtypeStruct(part.shape, jnp.float32),
        in_specs=[pl.BlockSpec(memory_space=pltpu.VMEM)],
        out_specs=pl.BlockSpec(memory_space=pltpu.VMEM),
        scratch_shapes=[
            pltpu.VMEM(block, jnp.float32),
            pltpu.VMEM(block[1:], jnp.float32),
            pltpu.VMEM(block, jnp.float32),
            pltpu.SemaphoreType.DMA((4, owners - 1)),
        ],
        compiler_params=pltpu.CompilerParams(collective_id=0, has_side_effects=True),
        name="mean_sums",
    )(part)


def return_kernel(owners, cols_ref, rows_ref, out_ref, landed, sems):
    me = lax.axis_index("dev")
    group = lax.axis_index("outer")
    beside = group + 1 - 2 * lax.rem(group, 2)
    opposite = 3 - group
    others = [lax.rem(me + step, owners) for step in range(1, owners)]
    peers = [{"dev": peer} for peer in others] + [{"outer": beside}, {"outer": opposite}]
    sources = [cols_ref.at[peer] for peer in others] + [rows_ref.at[1], rows_ref.at[2]]
    meet([(None, peer) for peer in peers], len(peers))
    copies = [
        pltpu.make_async_remote_copy(
            src_ref=sources[k],
            dst_ref=landed.at[k],
            send_sem=sems.at[0, k],
            recv_sem=sems.at[1, k],
            device_id=peers[k],
            device_id_type=MESH,
        )
        for k in range(len(peers))
    ]
    for copy in copies:
        copy.start()
    total = rows_ref[0]
    for k, copy in enumerate(copies):
        copy.wait_recv()
        total = total + landed[k]
    out_ref[...] = total
    for copy in copies:
        copy.wait_send()


def returned(cols, rows):
    owners = lax.axis_size("dev")
    peers = owners + 1
    return pl.pallas_call(
        functools.partial(return_kernel, owners),
        out_shape=jax.ShapeDtypeStruct(cols.shape[1:], jnp.float32),
        in_specs=[pl.BlockSpec(memory_space=pltpu.VMEM)] * 2,
        out_specs=pl.BlockSpec(memory_space=pltpu.VMEM),
        scratch_shapes=[
            pltpu.VMEM((peers,) + cols.shape[1:], jnp.float32),
            pltpu.SemaphoreType.DMA((2, peers)),
        ],
        compiler_params=pltpu.CompilerParams(collective_id=2, has_side_effects=True),
        name="return_sums",
    )(cols, rows)


PIECES = 4


def pair_kernel(
    unit_ref, lists_ref, gain_ref, klist_ref, kgain_ref,
    acc_ref, cols_ref, queries, keys, z_sems, core_sems, key_sems, side_sems,
):
    dev = lax.axis_index("dev")
    group = lax.axis_index("outer")
    z, core = dev // 2, lax.rem(dev, 2)
    rows = unit_ref.shape[0]
    piece = rows // PIECES
    partner = {"dev": 2 * z + 1 - core}
    above = {"dev": lax.rem(dev + 2, 8)}
    below = {"dev": lax.rem(dev + 6, 8)}
    beside = {"outer": group + 1 - 2 * lax.rem(group, 2)}
    across = {"outer": lax.rem(group + 2, 4)}
    meet(
        [(None, partner), (None, beside), (None, across), (z < 3, above), (z > 0, below)],
        3 + jnp.where(z < 3, 1, 0) + jnp.where(z > 0, 1, 0),
    )

    def part(k):
        return pl.ds(pl.multiple_of(k * piece, piece), piece)

    def remote(src, dst, send_sem, recv_sem, device):
        return pltpu.make_async_remote_copy(
            src_ref=src, dst_ref=dst, send_sem=send_sem, recv_sem=recv_sem,
            device_id=device, device_id_type=MESH,
        )

    def hop(unit, k, device, own=False):
        at = 2 * unit + core
        src = unit_ref.at[part(k)] if own else keys.at[at, part(k)]
        return remote(src, keys.at[at, part(k)], z_sems.at[unit, k], key_sems.at[at, k], device)

    def share(unit, k, own=False):
        at = 2 * unit + core
        src = unit_ref.at[part(k)] if own else keys.at[at, part(k)]
        return remote(
            src, keys.at[at, part(k)], core_sems.at[unit, k], key_sems.at[at, k], partner
        )

    def side(k):
        return remote(
            unit_ref.at[part(k)], queries.at[1, part(k)],
            side_sems.at[0, k], side_sems.at[1, k], beside,
        )

    def relay(k):
        return remote(
            queries.at[1, part(k)], queries.at[2, part(k)],
            side_sems.at[2, k], side_sems.at[3, k], across,
        )

    def arrived(at, k):
        remote(
            keys.at[at, part(k)], keys.at[at, part(k)],
            core_sems.at[0, k], key_sems.at[at, k], partner,
        ).wait_recv()

    def own_sends(k, act):
        act(side(k))

        @pl.when(z < 2)
        def _():
            act(hop(z, k, above, own=True))

        @pl.when(z == 3)
        def _():
            act(hop(z, k, below, own=True))

        act(share(z, k, own=True))

    def start(copy):
        copy.start()

    def sent(copy):
        copy.wait_send()

    def loop(body):
        lax.fori_loop(0, PIECES, lambda k, carry: (body(k), carry)[1], 0)

    loop(lambda k: own_sends(k, start))
    queries[0] = unit_ref[...]
    keys[dev] = unit_ref[...]
    acc_ref[...] = jnp.zeros_like(acc_ref)
    cols_ref[...] = jnp.zeros_like(cols_ref)

    def first(k):
        side(k).wait_recv()
        relay(k).start()

        @pl.when((z == 1) | (z == 2))
        def _():
            unit = z - 1
            arrived(2 * unit + core, k)
            hop(unit, k, above).start()
            share(unit, k).start()

        @pl.when(z == 2)
        def _():
            arrived(6 + core, k)
            share(3, k).start()

    loop(first)

    def late(k):
        @pl.when(z == 3)
        def _():
            arrived(2 + core, k)
            share(1, k).start()

        relay(k).wait_recv()

    loop(late)

    def stage(k):
        @pl.when(z >= 2)
        def _():
            arrived(core, k)
            share(0, k).start()

        @pl.when(z == 2)
        def _():
            hop(0, k, above).start()

        unit = jnp.where(
            k == 0, z, jnp.where(k == 1, jnp.where(z == 1, 0, 1), jnp.where(k == 2, 3, 0))
        )
        ready = (
            (k == 0)
            | ((k == 1) & (z > 0))
            | ((k == 2) & (z == 2))
            | ((k == 3) & (z >= 2))
        )

        @pl.when(ready)
        def _():
            loop(lambda p: arrived(2 * unit + 1 - core, p))
            foreign = jnp.where(k > 0, 1.0, 0.0)

            def one(c, carry):
                at = 2 * unit + c
                products = lax.dot_general(
                    queries[...].reshape(3 * rows, unit_ref.shape[1]),
                    keys[at],
                    (((1,), (1,)), ((), ())),
                    preferred_element_type=jnp.float32,
                )
                down = jnp.zeros((1, rows), jnp.float32)
                kl = klist_ref[at, 0]
                for b in range(3):
                    terms = jnp.exp(
                        0.5 * (gain_ref[b] + kgain_ref[at]) * products[b * rows : (b + 1) * rows]
                    )
                    wanted = lists_ref[b, 1] == kl
                    if b == 0:
                        wanted = wanted | (lists_ref[0, 2] == kl) | (lists_ref[0, 3] == kl)
                        shape = (rows, rows)
                        same = lax.broadcasted_iota(jnp.int32, shape, 0) == (
                            lax.broadcasted_iota(jnp.int32, shape, 1)
                        )
                        wanted = wanted & jnp.logical_not(same & (at == dev))
                        back = wanted
                    else:
                        back = lists_ref[b, 0] == klist_ref[at, b]
                    acc_ref[b] += jnp.where(wanted, terms, 0.0)
                    down = down + jnp.sum(jnp.where(back, terms, 0.0), axis=0, keepdims=True)
                cols_ref[at] = down * foreign
                return carry

            lax.fori_loop(0, 2, one, 0)

    loop(stage)

    def finish(k):
        own_sends(k, sent)
        sent(relay(k))

        @pl.when((z == 1) | (z == 2))
        def _():
            sent(hop(z - 1, k, above))
            sent(share(z - 1, k))

        @pl.when(z == 2)
        def _():
            sent(share(3, k))
            sent(hop(0, k, above))

        @pl.when(z == 3)
        def _():
            sent(share(1, k))

        @pl.when(z >= 2)
        def _():
            sent(share(0, k))

    loop(finish)


def paired(unit_rows, lists, gain, klists, kgain):
    rows, width = unit_rows.shape
    return pl.pallas_call(
        pair_kernel,
        out_shape=[
            jax.ShapeDtypeStruct((3, rows, rows), jnp.float32),
            jax.ShapeDtypeStruct((8, 1, rows), jnp.float32),
        ],
        in_specs=[pl.BlockSpec(memory_space=pltpu.VMEM)] * 5,
        out_specs=[pl.BlockSpec(memory_space=pltpu.VMEM)] * 2,
        scratch_shapes=[
            pltpu.VMEM((3, rows, width), jnp.bfloat16),
            pltpu.VMEM((8, rows, width), jnp.bfloat16),
            pltpu.SemaphoreType.DMA((4, PIECES)),
            pltpu.SemaphoreType.DMA((4, PIECES)),
            pltpu.SemaphoreType.DMA((8, PIECES)),
            pltpu.SemaphoreType.DMA((4, PIECES)),
        ],
        compiler_params=pltpu.CompilerParams(
            collective_id=1, has_side_effects=True, vmem_limit_bytes=56 * 1024 * 1024
        ),
        name="pairs",
    )(unit_rows, lists, gain, klists, kgain)


def lookup(table, index):
    hit = index[:, None] == jnp.arange(table.shape[0], dtype=jnp.int32)[None, :]
    return jnp.sum(jnp.where(hit, table[None, :], jnp.zeros((), table.dtype)), axis=1)


def gathered(documents, cluster_of, neighbours, sharpness):
    groups = lax.axis_size("outer")
    owners = lax.axis_size("dev")
    tokens_here, feature_width = documents.shape
    group_index = lax.axis_index("outer")
    owner_index = lax.axis_index("dev")
    clusters = groups * owners
    group_rows = owners * tokens_here
    cluster_range = jnp.arange(clusters, dtype=jnp.int32)
    sizes = jnp.sum((cluster_of[:, None] == cluster_range[None, :]).astype(jnp.int32), axis=0)

    def labels_at(group_at):
        start = (group_at * owners + owner_index) * tokens_here
        return lax.dynamic_slice_in_dim(cluster_of, start, tokens_here)

    own = labels_at(group_index)
    local = own - group_index * owners
    local_range = jnp.arange(owners, dtype=jnp.int32)
    member = (local_range[:, None] == local[None, :]).astype(jnp.bfloat16)
    sums = summed(jnp.dot(member, documents, preferred_element_type=jnp.float32))
    own_sizes = lax.dynamic_slice_in_dim(sizes, group_index * owners, owners)
    means = sums / own_sizes.astype(jnp.float32)[:, None]
    centre = jnp.dot(
        member.astype(jnp.float32).T,
        means,
        precision=lax.Precision.HIGHEST,
        preferred_element_type=jnp.float32,
    )
    centred = documents.astype(jnp.float32) - centre
    scaling = lax.rsqrt(jnp.mean(centred * centred, axis=1) + 1e-06) / math.sqrt(feature_width)
    unit_rows = (centred * scaling[:, None]).astype(jnp.bfloat16)

    even = group_index % 2 == 0
    beside = labels_at(group_index + 1 - 2 * (group_index % 2))
    across = labels_at(3 - group_index)
    before = neighbours[:, 2]
    after = neighbours[:, 3]
    seen_beside = jnp.where(even, before, after)
    seen_across = jnp.where(even, after, before)
    listed = [
        [own, own, lookup(neighbours[:, 0], own), lookup(neighbours[:, 1], own)],
        [beside] + [lookup(seen_beside, beside)] * 3,
        [across] + [lookup(seen_across, across)] * 3,
    ]
    lists = jnp.stack([jnp.stack(block) for block in listed])[..., None]
    gain = jnp.stack([lookup(sharpness, block[0]) for block in listed])[..., None]
    key_labels = lax.dynamic_slice_in_dim(cluster_of, group_index * group_rows, group_rows)
    key_shape = (owners, 1, 1, tokens_here)
    klists = jnp.concatenate(
        [
            key_labels.reshape(key_shape),
            lookup(seen_across, key_labels).reshape(key_shape),
            lookup(seen_beside, key_labels).reshape(key_shape),
        ],
        axis=1,
    )
    kgain = lookup(sharpness, key_labels).reshape(owners, 1, tokens_here)
    acc, cols = paired(unit_rows, lists, gain, klists, kgain)
    running = returned(cols, jnp.sum(acc, axis=2)[:, None, :])[0]
    counts = sizes - 1
    for position in range(neighbours.shape[1]):
        counts = counts + lookup(sizes, neighbours[:, position])
    return jnp.log(running / lookup(counts, own).astype(jnp.float32))


def solution(mesh):
    small = mesh.shape["dev"] == 8 and mesh.shape["outer"] == 4
    in_specs = (P(("outer", "dev"), None), P(), P(), P())
    out_specs = P(("outer", "dev"))
    body = gathered if small else shards
    return jax.shard_map(body, mesh=mesh, in_specs=in_specs, out_specs=out_specs, check_vma=False)
```

```python
import functools
import math

import jax
import jax.numpy as jnp
from jax import lax
from jax.experimental import pallas as pl
from jax.experimental.pallas import tpu as pltpu
from jax.sharding import PartitionSpec as P


def passed_along(block, axis, distance):
    devices = range(lax.axis_size(axis))
    route = [((i - distance) % len(devices), i) for i in devices]
    return lax.ppermute(block, axis, route)


def kernel_block(queries, others, pair_gain):
    products = jnp.einsum("qe,ke->qk", queries, others, preferred_element_type=jnp.float32)
    return jnp.exp(pair_gain * products)


def shards(documents, cluster_of, neighbours, sharpness):
    groups = lax.axis_size("outer")
    owners = lax.axis_size("dev")
    tokens_here = documents.shape[0]
    feature_width = documents.shape[1]
    capacity = max(2, 2 * tokens_here // owners)
    slot_count = owners * capacity
    group_index = lax.axis_index("outer")
    owner_index = lax.axis_index("dev")
    own_cluster = group_index * owners + owner_index
    block_labels = cluster_of.reshape(groups * owners, tokens_here)
    group_of_block = jnp.arange(groups * owners, dtype=jnp.int32) // owners
    local_labels = block_labels - group_of_block[:, None] * owners
    owner_range = jnp.arange(owners, dtype=jnp.int32)
    per_block = jnp.sum(
        (local_labels[:, :, None] == owner_range).astype(jnp.int32), axis=1
    ).reshape(groups, owners, owners)
    cluster_sizes = jnp.sum(per_block, axis=1).reshape(-1)
    own_labels = lax.dynamic_index_in_dim(local_labels, own_cluster, 0, keepdims=False)
    ordinal = jnp.arange(tokens_here, dtype=jnp.int32)
    earlier = ordinal[None, :] < ordinal[:, None]
    repeats = jnp.sum(
        ((own_labels[:, None] == own_labels[None, :]) & earlier).astype(jnp.int32), axis=1
    )
    target = own_labels * capacity + repeats
    placing = (jnp.arange(slot_count, dtype=jnp.int32)[:, None] == target[None, :]).astype(
        jnp.bfloat16
    )
    outgoing = jnp.dot(placing, documents, preferred_element_type=jnp.float32).astype(jnp.bfloat16)
    arrived = lax.all_to_all(
        outgoing.reshape(owners, capacity, feature_width),
        "dev",
        split_axis=0,
        concat_axis=0,
        tiled=True,
    ).reshape(slot_count, feature_width)

    def slot_mask(group_at, owner_at):
        senders = per_block[group_at, :, owner_at]
        return (
            (jnp.arange(capacity, dtype=jnp.int32)[None, :] < senders[:, None])
            .astype(jnp.float32)
            .reshape(-1)
        )

    present = slot_mask(group_index, owner_index)
    centre = jnp.dot(
        present.astype(jnp.bfloat16)[None, :], arrived, preferred_element_type=jnp.float32
    )[0]
    centre = centre / cluster_sizes[own_cluster].astype(jnp.float32)
    centred = arrived.astype(jnp.float32) - centre[None, :]
    scaling = lax.rsqrt(jnp.mean(centred * centred, axis=1) + 1e-06) / math.sqrt(feature_width)
    unit_rows = (centred * (scaling * present)[:, None]).astype(jnp.bfloat16)
    own_gain = sharpness[own_cluster]
    listed = neighbours[own_cluster]
    off_diagonal = 1.0 - jnp.eye(slot_count, dtype=jnp.float32)
    running = jnp.sum(
        kernel_block(unit_rows, unit_rows, own_gain) * (present[None, :] * off_diagonal), axis=1
    )
    beside = [passed_along(unit_rows, "dev", offset) for offset in (1, -1)]
    vertical = []
    for direction, position in ((1, 2), (-1, 3)):
        receiver_group = (group_index + direction) % groups
        wanted = neighbours[receiver_group * owners + owner_index, position]
        delta = (wanted % owners - owner_index + owners) % owners
        picked_rows = jnp.where(
            delta == 1, beside[1], jnp.where(delta == owners - 1, beside[0], unit_rows)
        )
        vertical.append(passed_along(picked_rows, "outer", direction))
    key_sets = [beside[0], beside[1], vertical[0], vertical[1]]
    for position in range(4):
        partner = listed[position]
        partner_group_at = partner // owners
        partner_owner_at = partner % owners
        partner_partner = partner_group_at * owners + partner_owner_at
        pair_gain = 0.5 * (own_gain + sharpness[partner_partner])
        partner = partner_partner
        kernel_terms = kernel_block(unit_rows, key_sets[position], pair_gain)
        key_mask = slot_mask(partner_group_at, partner_owner_at)
        running = running + jnp.sum(kernel_terms * key_mask[None, :], axis=1)
    partner_count = cluster_sizes[own_cluster] - 1 + jnp.sum(cluster_sizes[listed])
    slot_density = jnp.log(running / partner_count.astype(jnp.float32))
    answered = lax.all_to_all(
        slot_density.reshape(owners, capacity), "dev", split_axis=0, concat_axis=0, tiled=True
    ).reshape(-1)
    return answered[target]


MESH = pl.DeviceIdType.MESH


def meet(peers, expected):
    barrier = pltpu.get_barrier_semaphore()
    for present, peer in peers:
        if present is None:
            pl.semaphore_signal(barrier, inc=1, device_id=peer, device_id_type=MESH)
        else:

            @pl.when(present)
            def _(peer=peer):
                pl.semaphore_signal(barrier, inc=1, device_id=peer, device_id_type=MESH)

    pl.semaphore_wait(barrier, expected)


def sum_kernel(owners, part_ref, out_ref, landed, reduced, gathered_sums, sems):
    me = lax.axis_index("dev")
    width = part_ref.shape[1] // owners

    def span(at):
        return pl.ds(pl.multiple_of(at * width, 128), width)

    others = [lax.rem(me + step, owners) for step in range(1, owners)]
    meet([(None, {"dev": peer}) for peer in others], owners - 1)

    def scatter(step):
        return pltpu.make_async_remote_copy(
            src_ref=part_ref.at[:, span(others[step])],
            dst_ref=landed.at[step],
            send_sem=sems.at[0, step],
            recv_sem=sems.at[1, step],
            device_id={"dev": others[step]},
            device_id_type=MESH,
        )

    def spread(step):
        return pltpu.make_async_remote_copy(
            src_ref=reduced,
            dst_ref=gathered_sums.at[step],
            send_sem=sems.at[2, step],
            recv_sem=sems.at[3, step],
            device_id={"dev": others[step]},
            device_id_type=MESH,
        )

    for step in range(owners - 1):
        scatter(step).start()
    total = part_ref[:, span(me)]
    for step in range(owners - 1):
        scatter(step).wait_recv()
        total = total + landed[step]
    reduced[...] = total
    for step in range(owners - 1):
        spread(step).start()
    out_ref[:, span(me)] = total
    for step in range(owners - 1):
        spread(step).wait_recv()
        sender = lax.rem(me + owners - 1 - step, owners)
        out_ref[:, span(sender)] = gathered_sums[step]
    for step in range(owners - 1):
        scatter(step).wait_send()
        spread(step).wait_send()


def summed(part):
    owners = lax.axis_size("dev")
    rows, width = part.shape
    block = (owners - 1, rows, width // owners)
    return pl.pallas_call(
        functools.partial(sum_kernel, owners),
        out_shape=jax.ShapeDtypeStruct(part.shape, jnp.float32),
        in_specs=[pl.BlockSpec(memory_space=pltpu.VMEM)],
        out_specs=pl.BlockSpec(memory_space=pltpu.VMEM),
        scratch_shapes=[
            pltpu.VMEM(block, jnp.float32),
            pltpu.VMEM(block[1:], jnp.float32),
            pltpu.VMEM(block, jnp.float32),
            pltpu.SemaphoreType.DMA((4, owners - 1)),
        ],
        compiler_params=pltpu.CompilerParams(collective_id=0, has_side_effects=True),
        name="mean_sums",
    )(part)


def return_kernel(owners, cols_ref, rows_ref, out_ref, landed, sems):
    me = lax.axis_index("dev")
    group = lax.axis_index("outer")
    beside = group + 1 - 2 * lax.rem(group, 2)
    opposite = 3 - group
    others = [lax.rem(me + step, owners) for step in range(1, owners)]
    peers = [{"dev": peer} for peer in others] + [{"outer": beside}, {"outer": opposite}]
    sources = [cols_ref.at[peer] for peer in others] + [rows_ref.at[1], rows_ref.at[2]]
    meet([(None, peer) for peer in peers], len(peers))
    copies = [
        pltpu.make_async_remote_copy(
            src_ref=sources[k],
            dst_ref=landed.at[k],
            send_sem=sems.at[0, k],
            recv_sem=sems.at[1, k],
            device_id=peers[k],
            device_id_type=MESH,
        )
        for k in range(len(peers))
    ]
    for copy in copies:
        copy.start()
    total = rows_ref[0]
    for k, copy in enumerate(copies):
        copy.wait_recv()
        total = total + landed[k]
    out_ref[...] = total
    for copy in copies:
        copy.wait_send()


def returned(cols, rows):
    owners = lax.axis_size("dev")
    peers = owners + 1
    return pl.pallas_call(
        functools.partial(return_kernel, owners),
        out_shape=jax.ShapeDtypeStruct(cols.shape[1:], jnp.float32),
        in_specs=[pl.BlockSpec(memory_space=pltpu.VMEM)] * 2,
        out_specs=pl.BlockSpec(memory_space=pltpu.VMEM),
        scratch_shapes=[
            pltpu.VMEM((peers,) + cols.shape[1:], jnp.float32),
            pltpu.SemaphoreType.DMA((2, peers)),
        ],
        compiler_params=pltpu.CompilerParams(collective_id=2, has_side_effects=True),
        name="return_sums",
    )(cols, rows)


PIECES = 6


def pair_kernel(
    unit_ref, labels_ref, neighbours_ref, sharpness_ref, rows_ref, cols_ref,
    lists_ref, gain_ref, klist_ref, kgain_ref, acc_ref,
    queries, keys, z_sems, core_sems, key_sems, side_sems,
):
    dev = lax.axis_index("dev")
    group = lax.axis_index("outer")
    z, core = dev // 2, lax.rem(dev, 2)
    rows = unit_ref.shape[0]
    piece = rows // PIECES
    partner = {"dev": 2 * z + 1 - core}
    above = {"dev": lax.rem(dev + 2, 8)}
    below = {"dev": lax.rem(dev + 6, 8)}
    beside = {"outer": group + 1 - 2 * lax.rem(group, 2)}
    across = {"outer": lax.rem(group + 2, 4)}
    meet(
        [(None, partner), (None, beside), (None, across), (z < 3, above), (z > 0, below)],
        3 + jnp.where(z < 3, 1, 0) + jnp.where(z > 0, 1, 0),
    )

    def part(k):
        return pl.ds(pl.multiple_of(k * piece, piece), piece)

    def remote(src, dst, send_sem, recv_sem, device):
        return pltpu.make_async_remote_copy(
            src_ref=src, dst_ref=dst, send_sem=send_sem, recv_sem=recv_sem,
            device_id=device, device_id_type=MESH,
        )

    def hop(unit, k, device, own=False):
        at = 2 * unit + core
        src = unit_ref.at[part(k)] if own else keys.at[at, part(k)]
        return remote(src, keys.at[at, part(k)], z_sems.at[unit, k], key_sems.at[at, k], device)

    def share(unit, k, own=False):
        at = 2 * unit + core
        src = unit_ref.at[part(k)] if own else keys.at[at, part(k)]
        return remote(
            src, keys.at[at, part(k)], core_sems.at[unit, k], key_sems.at[at, k], partner
        )

    def side(k):
        return remote(
            unit_ref.at[part(k)], queries.at[1, part(k)],
            side_sems.at[0, k], side_sems.at[1, k], beside,
        )

    def relay(k):
        return remote(
            queries.at[1, part(k)], queries.at[2, part(k)],
            side_sems.at[2, k], side_sems.at[3, k], across,
        )

    def arrived(at, k):
        remote(
            keys.at[at, part(k)], keys.at[at, part(k)],
            core_sems.at[0, k], key_sems.at[at, k], partner,
        ).wait_recv()

    def own_sends(k, act):
        act(side(k))

        @pl.when(z < 2)
        def _():
            act(hop(z, k, above, own=True))

        @pl.when(z == 3)
        def _():
            act(hop(z, k, below, own=True))

        act(share(z, k, own=True))

    def start(copy):
        copy.start()

    def sent(copy):
        copy.wait_send()

    def loop(body):
        lax.fori_loop(0, PIECES, lambda k, carry: (body(k), carry)[1], 0)

    loop(lambda k: own_sends(k, start))
    square = (rows, rows)
    same = lax.broadcasted_iota(jnp.int32, square, 0) == lax.broadcasted_iota(jnp.int32, square, 1)

    def chosen(read, labels, base, zero):
        found = jnp.full(labels.shape, zero, jnp.float32)
        for h in range(8):
            found = jnp.where(labels == base + h, read(base + h), found)
        return found

    def listed(position):
        return lambda c: neighbours_ref[c, position].astype(jnp.float32)

    def sharp(c):
        return sharpness_ref[c]

    def upright(row):
        return jnp.sum(jnp.where(same, row, 0.0), axis=1, keepdims=True)

    odd = lax.rem(group, 2)
    toward = {0: None, 1: 2 + odd, 2: 3 - odd}
    for b, at_group in enumerate((group, group + 1 - 2 * odd, 3 - group)):
        base = at_group * 8
        labels = labels_ref[base + dev]
        lists_ref[b, 0] = upright(labels.astype(jnp.float32))
        gain_ref[b] = upright(chosen(sharp, labels, base, 0.0))
        positions = (0, 1) if b == 0 else (toward[b],)
        for slot, position in enumerate(positions):
            lists_ref[b, 1 + slot] = upright(chosen(listed(position), labels, base, 0.0))

    def key_tables(at):
        labels = labels_ref[group * 8 + at]
        klist_ref[at, 0] = labels.astype(jnp.float32)
        kgain_ref[at] = chosen(sharp, labels, group * 8, 0.0)
        klist_ref[at, 1] = chosen(listed(3 - odd), labels, group * 8, 0.0)
        klist_ref[at, 2] = chosen(listed(2 + odd), labels, group * 8, 0.0)

    lax.fori_loop(0, 8, lambda at, carry: (key_tables(at), carry)[1], 0)
    queries[0] = unit_ref[...]
    keys[dev] = unit_ref[...]
    acc_ref[...] = jnp.zeros_like(acc_ref)
    cols_ref[...] = jnp.zeros_like(cols_ref)

    def first(k):
        side(k).wait_recv()
        relay(k).start()

        @pl.when((z == 1) | (z == 2))
        def _():
            unit = z - 1
            arrived(2 * unit + core, k)
            hop(unit, k, above).start()
            share(unit, k).start()

        @pl.when(z == 2)
        def _():
            arrived(6 + core, k)
            share(3, k).start()

    loop(first)

    def late(k):
        @pl.when(z == 3)
        def _():
            arrived(2 + core, k)
            share(1, k).start()

        relay(k).wait_recv()

    loop(late)

    def stage(k):
        @pl.when(z >= 2)
        def _():
            arrived(core, k)
            share(0, k).start()

        @pl.when(z == 2)
        def _():
            hop(0, k, above).start()

        unit = jnp.where(
            k == 0, z, jnp.where(k == 1, jnp.where(z == 1, 0, 1), jnp.where(k == 2, 3, 0))
        )
        ready = (
            (k == 0)
            | ((k == 1) & (z > 0))
            | ((k == 2) & (z == 2))
            | ((k == PIECES - 1) & (z >= 2))
        )

        @pl.when(ready)
        def _():
            loop(lambda p: arrived(2 * unit + 1 - core, p))
            foreign = jnp.where(k > 0, 1.0, 0.0)

            def one(c, carry):
                at = 2 * unit + c
                products = lax.dot_general(
                    queries[...].reshape(3 * rows, unit_ref.shape[1]),
                    keys[at],
                    (((1,), (1,)), ((), ())),
                    preferred_element_type=jnp.float32,
                )
                down = jnp.zeros((1, rows), jnp.float32)
                kl = klist_ref[at, 0]
                for b in range(3):
                    terms = jnp.exp(
                        0.5 * (gain_ref[b] + kgain_ref[at]) * products[b * rows : (b + 1) * rows]
                    )
                    wanted = lists_ref[b, 1] == kl
                    if b == 0:
                        wanted = wanted | (lists_ref[0, 2] == kl) | (lists_ref[0, 0] == kl)
                        wanted = wanted & jnp.logical_not(same & (at == dev))
                        back = wanted
                    else:
                        back = lists_ref[b, 0] == klist_ref[at, b]
                    acc_ref[b] += jnp.where(wanted, terms, 0.0)
                    down = down + jnp.sum(jnp.where(back, terms, 0.0), axis=0, keepdims=True)
                cols_ref[at] = down * foreign
                return carry

            lax.fori_loop(0, 2, one, 0)

    loop(stage)
    for b in range(3):
        across_lanes = jnp.sum(acc_ref[b], axis=1, keepdims=True)
        rows_ref[b] = jnp.sum(jnp.where(same, across_lanes, 0.0), axis=0, keepdims=True)

    def finish(k):
        own_sends(k, sent)
        sent(relay(k))

        @pl.when((z == 1) | (z == 2))
        def _():
            sent(hop(z - 1, k, above))
            sent(share(z - 1, k))

        @pl.when(z == 2)
        def _():
            sent(share(3, k))
            sent(hop(0, k, above))

        @pl.when(z == 3)
        def _():
            sent(share(1, k))

        @pl.when(z >= 2)
        def _():
            sent(share(0, k))

    loop(finish)


def paired(unit_rows, labels, neighbours, sharpness):
    rows, width = unit_rows.shape
    vmem = pl.BlockSpec(memory_space=pltpu.VMEM)
    smem = pl.BlockSpec(memory_space=pltpu.SMEM)
    return pl.pallas_call(
        pair_kernel,
        out_shape=[
            jax.ShapeDtypeStruct((3, 1, rows), jnp.float32),
            jax.ShapeDtypeStruct((8, 1, rows), jnp.float32),
        ],
        in_specs=[vmem, vmem, smem, smem],
        out_specs=[vmem, vmem],
        scratch_shapes=[
            pltpu.VMEM((3, 3, rows, 1), jnp.float32),
            pltpu.VMEM((3, rows, 1), jnp.float32),
            pltpu.VMEM((8, 3, 1, rows), jnp.float32),
            pltpu.VMEM((8, 1, rows), jnp.float32),
            pltpu.VMEM((3, rows, rows), jnp.float32),
            pltpu.VMEM((3, rows, width), jnp.bfloat16),
            pltpu.VMEM((8, rows, width), jnp.bfloat16),
            pltpu.SemaphoreType.DMA((4, PIECES)),
            pltpu.SemaphoreType.DMA((4, PIECES)),
            pltpu.SemaphoreType.DMA((8, PIECES)),
            pltpu.SemaphoreType.DMA((4, PIECES)),
        ],
        compiler_params=pltpu.CompilerParams(
            collective_id=1, has_side_effects=True, vmem_limit_bytes=56 * 1024 * 1024
        ),
        name="pairs",
    )(unit_rows, labels, neighbours, sharpness)


def lookup(table, index):
    hit = index[:, None] == jnp.arange(table.shape[0], dtype=jnp.int32)[None, :]
    return jnp.sum(jnp.where(hit, table[None, :], jnp.zeros((), table.dtype)), axis=1)


def gathered(documents, cluster_of, neighbours, sharpness):
    groups = lax.axis_size("outer")
    owners = lax.axis_size("dev")
    tokens_here, feature_width = documents.shape
    group_index = lax.axis_index("outer")
    owner_index = lax.axis_index("dev")
    clusters = groups * owners
    cluster_range = jnp.arange(clusters, dtype=jnp.int32)
    sizes = jnp.sum((cluster_of[:, None] == cluster_range[None, :]).astype(jnp.int32), axis=0)

    def labels_at(group_at):
        start = (group_at * owners + owner_index) * tokens_here
        return lax.dynamic_slice_in_dim(cluster_of, start, tokens_here)

    own = labels_at(group_index)
    local = own - group_index * owners
    local_range = jnp.arange(owners, dtype=jnp.int32)
    member = (local_range[:, None] == local[None, :]).astype(jnp.bfloat16)
    sums = summed(jnp.dot(member, documents, preferred_element_type=jnp.float32))
    own_sizes = lax.dynamic_slice_in_dim(sizes, group_index * owners, owners)
    means = sums / own_sizes.astype(jnp.float32)[:, None]
    centre = jnp.dot(
        member.astype(jnp.float32).T,
        means,
        precision=lax.Precision.HIGHEST,
        preferred_element_type=jnp.float32,
    )
    centred = documents.astype(jnp.float32) - centre
    scaling = lax.rsqrt(jnp.mean(centred * centred, axis=1) + 1e-06) / math.sqrt(feature_width)
    unit_rows = (centred * scaling[:, None]).astype(jnp.bfloat16)

    labels = cluster_of.reshape(clusters, 1, tokens_here)
    rows, cols = paired(unit_rows, labels, neighbours, sharpness)
    running = returned(cols, rows)[0]
    counts = sizes - 1
    for position in range(neighbours.shape[1]):
        counts = counts + lookup(sizes, neighbours[:, position])
    return jnp.log(running / lookup(counts, own).astype(jnp.float32))


def solution(mesh):
    small = mesh.shape["dev"] == 8 and mesh.shape["outer"] == 4
    in_specs = (P(("outer", "dev"), None), P(), P(), P())
    out_specs = P(("outer", "dev"))
    body = gathered if small else shards
    return jax.shard_map(body, mesh=mesh, in_specs=in_specs, out_specs=out_specs, check_vma=False)
```
